32 devices in a mesh: seq: 8 (over z, x), head: 4 (over y, core).
Axes of the slice: x: 2, y: 2, z: 4, core: 2. Of those that a mesh axis runs over, the one named last changes fastest.
Arguments:
- xs: bfloat16 [8192, 4096], P('seq', 'head'), may hold values from -6 to 6
- gate_branch: bfloat16 [8192, 4096], P('seq', 'head'), may hold values from -6 to 6
- bmat: bfloat16 [8192, 128], P('seq'), may hold values from -0.375 to 0.375
- cmat: bfloat16 [8192, 128], P('seq'), may hold values from -0.375 to 0.375
- dt_code: int32 [64, 8192], P('head', 'seq'), may hold values from 1 to 32768
- resets: int32 [8192], P('seq'), may hold values 0 or 1
- decay_rate: float32 [64], P('head'), may hold values from 4.8828125e-05 to 0.08, as said below
- skip: float32 [64], P('head'), may hold values from 0.5 to 1.5
- norm_gain: float32 [4096], P('head'), may hold values from 0.1 to 1.9
- out_weight: bfloat16 [4096, 4096], P('head'), may hold values from -0.09375 to 0.09375
Outputs:
- mixed: bfloat16 [8192, 4096], P(('seq', 'head'))
The draws below stay inside these ranges and needn't reach their ends.
Inputs may be any that keep to these rules, and one draw needn't show every extreme that they name: `decay_rate`: positive rates.
All inputs are finite; a program needn't handle non-finite values. No bound on the sum of `resets` on one device may be relied on, other than what follows from the above.
Results may differ from the reference program's by a relative error of at most 0.023.
Values may be sent and summed in bfloat16 or wider, within the bound.
A program may use at most 128 MiB of HBM per device.

```python
import jax
import jax.numpy as jnp
from jax import lax

D = 4096
HEADS = 64
HEAD_DIM = 64
STATE = 128
SPAN = 256
HORIZON_TICKS = 8192
INNER = 4096
GROUPS = 4


def draw_xs(key, part):
    first = jax.random.fold_in(key, 0)
    values = jax.random.normal(first, (HORIZON_TICKS, INNER), jnp.float32)
    return jnp.clip(values, -6.0, 6.0).astype(jnp.bfloat16)


def draw_dt_code(key, part):
    first, right_factor = jax.random.split(jax.random.fold_in(key, 11))
    starting_displacement = jax.random.randint(first, (HEADS, HORIZON_TICKS), 1, 17)
    contiguous_span_count = jax.random.randint(right_factor, (HORIZON_TICKS,), 0, HORIZON_TICKS) < 3
    return jnp.where(contiguous_span_count[None, :], 4 * HORIZON_TICKS, starting_displacement).astype(jnp.int32)


def draw_decay_rate(key, part):
    first, right_factor, third = jax.random.split(jax.random.fold_in(key, 23), 3)
    share = 0.5
    slow_mask = jax.random.uniform(first, (HEADS,), jnp.float32) < share
    slow_rate = jnp.exp(jax.random.uniform(right_factor, (HEADS,), jnp.float32, jnp.log(0.4), jnp.log(1.6))) / HORIZON_TICKS
    fast_rate = jnp.exp(jax.random.uniform(third, (HEADS,), jnp.float32, jnp.log(0.03), jnp.log(0.08)))
    return jnp.where(slow_mask, slow_rate, fast_rate).astype(jnp.float32)


def place_ends(drawn, key, low, high):
    longest = drawn.shape.index(max(drawn.shape))
    spots = []
    for shift in (0, 1):
        where = [jax.random.randint(jax.random.fold_in(key, axis), (), 0, length) for axis, length in enumerate(drawn.shape)]
        where[longest] = (where[longest] + shift) % drawn.shape[longest]
        spots.append(tuple(where))
    return drawn.at[spots[0]].set(low).at[spots[1]].set(high)


def shard_levels(rng, shape, shards, low, top_value):
    level, own = 1.0, jax.random.fold_in(rng, 6)
    for dim, parts in shards:
        draws = jnp.exp(jax.random.uniform(jax.random.fold_in(own, dim), (parts,), jnp.float32, low / len(shards), top_value / len(shards)))
        level = level * jnp.repeat(draws, shape[dim] // parts).reshape([-1 if axis == dim else 1 for axis in range(len(shape))])
    return level


def centred(own_key, shape, spread, reach, cuts=(), kind=jnp.bfloat16):
    entries = spread * jax.random.normal(own_key, shape, jnp.float32)
    if cuts:
        entries = entries * shard_levels(own_key, shape, cuts, -0.22, 0.18)
    return jnp.clip(entries, -reach, reach).astype(kind)


def setup_inputs(seed: int = 0) -> dict:
    key_of = jax.random.split(jax.random.key(seed), 11)
    xs = draw_xs(jax.random.fold_in(key_of[10], 71), 0)
    gate_branch = centred(key_of[1], (HORIZON_TICKS, INNER), 1.0, 6.0, ((0, 8), (1, 4)))
    bmat = centred(key_of[2], (HORIZON_TICKS, STATE), (2 * (HORIZON_TICKS * STATE) ** -0.25), 0.375, ((0, 8),))
    cmat = centred(key_of[3], (HORIZON_TICKS, STATE), (2 * (HORIZON_TICKS * STATE) ** -0.25), 0.375, ((0, 8),))
    dt_code = draw_dt_code(jax.random.fold_in(key_of[10], 71), 0)
    resets = place_ends((jax.random.randint(key_of[5], (HORIZON_TICKS,), 0, HORIZON_TICKS) < 2).astype(jnp.int32), jax.random.fold_in(key_of[5], 1), 0, 1)
    decay_rate = draw_decay_rate(jax.random.fold_in(key_of[10], 71), 0)
    skip = jnp.clip(0.5 + 1.0 * jax.random.uniform(key_of[7], (HEADS,), jnp.float32) ** shard_levels(key_of[7], (HEADS,), ((0, 4),), -0.2, 0.2), 0.5, 1.5)
    norm_gain = jnp.clip(1.0 + 0.18 * jax.random.normal(key_of[8], (INNER,), jnp.float32), 0.1, 1.9)
    out_weight = centred(key_of[9], (INNER, D), INNER ** -0.5, 0.09375, ((0, 4),))
    return {"xs": xs, "gate_branch": gate_branch, "bmat": bmat, "cmat": cmat, "dt_code": dt_code, "resets": resets, "decay_rate": decay_rate, "skip": skip, "norm_gain": norm_gain, "out_weight": out_weight}


def reference(xs, gate_branch, bmat, cmat, dt_code, resets, decay_rate, skip, norm_gain, out_weight):
    step_size = dt_code.astype(jnp.float32) / 16.0
    input_scale = jnp.minimum(step_size, 1.0)
    logarithmic_damping = -decay_rate[:, None] * step_size
    blocks = HORIZON_TICKS // SPAN
    values = xs.reshape(blocks, SPAN, HEADS, HEAD_DIM)
    key_blocks = bmat.reshape(blocks, SPAN, STATE)
    query_blocks = cmat.reshape(blocks, SPAN, STATE)
    log_blocks = logarithmic_damping.reshape(HEADS, blocks, SPAN).transpose(1, 0, 2)
    scale_blocks = input_scale.reshape(HEADS, blocks, SPAN).transpose(1, 0, 2)
    flag_blocks = resets.reshape(blocks, SPAN)

    def propagate_forward(state, inputs):
        value, key_rows, query, logs, scales, flags = inputs
        cumulative = jnp.cumsum(logs, axis=1)
        counts = jnp.cumsum(flags)
        position = jnp.arange(SPAN)
        linked = (counts[:, None] == counts[None, :]) & (position[None, :] <= position[:, None])
        gaps = jnp.where(linked[None], cumulative[:, :, None] - cumulative[:, None, :], 0.0)
        within = jnp.where(linked[None], jnp.exp(gaps), 0.0)
        intersection = jnp.dot(query, key_rows.T, preferred_element_type=jnp.float32)
        value_float = value.astype(jnp.float32)
        scaled = (value_float * scales.T[:, :, None]).astype(jnp.bfloat16)
        scaled_float = lax.optimization_barrier(scaled).astype(jnp.float32)
        scores = (within * intersection[None]).astype(jnp.bfloat16)
        scores_float = lax.optimization_barrier(scores).astype(jnp.float32)
        output = jnp.einsum('hij,jhp->ihp', scores_float, scaled_float, precision=lax.Precision.HIGHEST)
        from_start = jnp.where(counts[None, :] == 0, jnp.exp(cumulative), 0.0)
        query_float = query.astype(jnp.float32)
        carried = jnp.einsum('in,hpn->ihp', query_float, state, precision=lax.Precision.HIGHEST)
        output = output + carried * from_start.T[:, :, None]
        to_end = jnp.where(counts[None, :] == counts[-1], jnp.exp(cumulative[:, -1:] - cumulative), 0.0)
        through = jnp.where(counts[-1] == 0, jnp.exp(cumulative[:, -1]), 0.0)
        weighted = (scaled_float * to_end.T[:, :, None]).astype(jnp.bfloat16)
        weighted_float = lax.optimization_barrier(weighted).astype(jnp.float32)
        fresh = jnp.einsum('jhp,jn->hpn', weighted_float, key_rows.astype(jnp.float32), precision=lax.Precision.HIGHEST)
        state = through[:, None, None] * state + fresh
        output = output + skip[None, :, None] * value_float
        return (state, output)
    initial = jnp.zeros((HEADS, HEAD_DIM, STATE), jnp.float32)
    outputs = lax.scan(propagate_forward, initial, (values, key_blocks, query_blocks, log_blocks, scale_blocks, flag_blocks))[1]
    ssm_out = outputs.reshape(HORIZON_TICKS, INNER)
    gated = ssm_out * jax.nn.silu(gate_branch.astype(jnp.float32))
    mean_square = lax.optimization_barrier(jnp.mean(gated * gated, axis=1, keepdims=True))
    hidden = (gated * lax.rsqrt(mean_square + 1e-05) * norm_gain[None, :]).astype(jnp.bfloat16)
    group_width = INNER // GROUPS
    summed = jnp.zeros((HORIZON_TICKS, D), jnp.float32)
    for group in range(GROUPS):
        lower = group * group_width
        partial_value = jnp.dot(hidden[:, lower:lower + group_width], out_weight[lower:lower + group_width], preferred_element_type=jnp.float32).astype(jnp.bfloat16)
        summed = summed + lax.optimization_barrier(partial_value).astype(jnp.float32)
    return summed.astype(jnp.bfloat16)
```

```python
import functools

import jax
import jax.numpy as jnp
from jax import lax
from jax.experimental import pallas as pl
from jax.experimental.pallas import tpu as pltpu
from jax.sharding import PartitionSpec as P

HEAD_DIM = 64
SPAN = 256
CHUNKS = 8
EARLY = 3
F32 = jnp.float32
BF16 = jnp.bfloat16
MESH = pl.DeviceIdType.MESH
VMEM_BYTES = 60 * 1024 * 1024
LOG2E = 1.4426950408889634


def dot_nt(a, b):
    return lax.dot_general(a, b, (((1,), (1,)), ((), ())), preferred_element_type=F32)


def dot_tn(a, b):
    return lax.dot_general(a, b, (((0,), (0,)), ((), ())), preferred_element_type=F32)


def dot_nn(a, b):
    return jnp.dot(a, b, preferred_element_type=F32)


def two_pieces(v):
    high = v.astype(BF16)
    low = (v - high.astype(F32)).astype(BF16)
    return jnp.concatenate([high, low], axis=1)


def spread(heads):
    rows = lax.broadcasted_iota(jnp.int32, (2 * heads, heads * HEAD_DIM), 0)
    columns = lax.broadcasted_iota(jnp.int32, (2 * heads, heads * HEAD_DIM), 1)
    own = (columns // HEAD_DIM == rows) | (columns // HEAD_DIM == rows - heads)
    return jnp.where(own, 1.0, 0.0).astype(BF16)


def digits(code, flags):
    low = code & 127
    middle = (code >> 7) & 127
    high = code >> 14
    extra = jnp.broadcast_to(flags, code.shape)
    rows = jnp.concatenate([low, middle, high, extra], axis=0)
    return rows.astype(F32).astype(BF16)


def joined(sums, heads, axis):
    def take(n):
        return lax.slice_in_dim(sums, n * heads, (n + 1) * heads, axis=axis)

    return (take(0) + 128.0 * take(1) + 16384.0 * take(2)), take(3)


def layer_kernel(
    shards, x_hbm, gate_hbm, b_ref, c_ref, code_ref, flag_ref, rate_ref, skip_ref, gain_ref, w_hbm, out_ref,
    x_ref, gate_ref, w, scaled, cross, columns_of, rows_of, fall, eyes, skips, gains, reach, local, ssm, mine, squares,
    own, final, other_final, decay, other_decay, came, passed, starts,
    kept, send1, recv1, send2, recv2, sq_send, sq_recv,
    x_sem, g_sem, w_sem, fs, fr, ds, dr, cs, cr, s1, r1, s2, r2, sqs, sqr,
):
    me = lax.axis_index("head")
    rank = lax.axis_index("seq")
    core = me % 2
    half = me // 2
    partner = half * 2 + (1 - core)
    across = (1 - half) * 2 + core
    diagonal = (1 - half) * 2 + (1 - core)
    odd = rank % 2
    twin = rank + 1 - 2 * odd
    level = rank // 2
    ticks, inner = x_ref.shape
    heads = code_ref.shape[0]
    width = out_ref.shape[1] // CHUNKS
    blocks = ticks // SPAN
    pieces = heads // 2
    lanes = 2 * HEAD_DIM
    lower = SPAN // 2

    def load_x(n):
        rows = pl.ds(n * SPAN, SPAN)
        return pltpu.make_async_copy(x_hbm.at[rows], x_ref.at[rows], x_sem.at[n])

    def load_gate(n):
        rows = pl.ds(n * SPAN, SPAN)
        return pltpu.make_async_copy(gate_hbm.at[rows], gate_ref.at[rows], g_sem.at[n])

    def load(n):
        return pltpu.make_async_copy(w_hbm.at[:, pl.ds(n * width, width)], w.at[n], w_sem.at[n])

    for n in range(blocks):
        load_x(n).start()
    for n in range(blocks):
        load_gate(n).start()
    for n in range(CHUNKS):
        load(n).start()

    barrier = pltpu.get_barrier_semaphore()
    for other in (partner, across, diagonal):
        pl.semaphore_signal(barrier, inc=1, device_id={"head": other}, device_id_type=MESH)
    for other in (twin, (rank + 2) % shards, (rank + shards - 2) % shards):
        pl.semaphore_signal(barrier, inc=1, device_id={"seq": other}, device_id_type=MESH)

    eye = spread(heads)
    rate_row = rate_ref[...] * (LOG2E / 16.0)
    hi = lax.broadcasted_iota(jnp.int32, (heads, heads), 0)
    hj = lax.broadcasted_iota(jnp.int32, (heads, heads), 1)
    rate_col = jnp.sum(jnp.where(hi == hj, rate_row, 0.0), axis=1, keepdims=True)
    si = lax.broadcasted_iota(jnp.int32, (SPAN, SPAN), 0)
    sj = lax.broadcasted_iota(jnp.int32, (SPAN, SPAN), 1)

    def scales(codes):
        return jnp.transpose(jnp.minimum(codes.astype(F32) / 16.0, 1.0))

    def local_states():
        ti = lax.broadcasted_iota(jnp.int32, (SPAN + 8, SPAN), 0)
        tj = lax.broadcasted_iota(jnp.int32, (SPAN + 8, SPAN), 1)
        later = jnp.where((tj > ti) | (ti >= SPAN), 1.0, 0.0).astype(BF16)
        factors, last = [], []
        for n in range(blocks):
            tokens = slice(n * SPAN, (n + 1) * SPAN)
            codes = code_ref[:, tokens]
            after, seen = joined(dot_nt(later, digits(codes, flag_ref[:, tokens])), heads, 1)
            kept_on = jnp.where(seen == 0.0, jnp.exp2(-rate_row * after), 0.0)
            factors.append(kept_on[0:SPAN] * scales(codes))
            last.append(kept_on[SPAN : SPAN + 1])
        so_far = [jnp.ones_like(last[0])]
        for n in range(blocks):
            so_far.append(so_far[-1] * last[n])
        stack = so_far + last
        stack = stack + [so_far[0]] * (16 - len(stack))
        wide_rows = dot_nn(two_pieces(jnp.concatenate(stack, axis=0)), eye)
        state = None
        for n in range(blocks):
            tokens = slice(n * SPAN, (n + 1) * SPAN)
            wide = dot_nn(two_pieces(factors[n]), eye)
            load_x(n).wait()
            weighted = (x_ref[tokens, :].astype(F32) * wide).astype(BF16)
            fresh = dot_tn(b_ref[tokens, :], weighted)
            if n > 0:
                for q in range(pieces):
                    local[n, q] = state[:, q * lanes : (q + 1) * lanes]
                fresh = fresh + wide_rows[blocks + 1 + n : blocks + 2 + n] * state
            state = fresh
        for q in range(pieces):
            part = slice(q * lanes, (q + 1) * lanes)
            own[q] = state[:, part]
            final[q] = state[:, part].astype(BF16)
            local[0, q] = jnp.zeros((local.shape[2], lanes), F32)
            decay[q] = wide_rows[blocks : blocks + 1, part]
            for n in range(blocks):
                reach[n, q] = wide_rows[n : n + 1, part]

    def final_copy(q):
        return pltpu.make_async_remote_copy(
            src_ref=final.at[q], dst_ref=other_final.at[q], send_sem=fs.at[q],
            recv_sem=fr.at[q], device_id={"seq": twin}, device_id_type=MESH,
        )

    def decay_copy():
        return pltpu.make_async_remote_copy(
            src_ref=decay, dst_ref=other_decay, send_sem=ds.at[0],
            recv_sem=dr.at[0], device_id={"seq": twin}, device_id_type=MESH,
        )

    def chain_copy(q):
        return pltpu.make_async_remote_copy(
            src_ref=passed.at[q], dst_ref=came.at[q], send_sem=cs.at[q],
            recv_sem=cr.at[q], device_id={"seq": (rank + 2) % shards}, device_id_type=MESH,
        )

    def square_copy(slot, other):
        return pltpu.make_async_remote_copy(
            src_ref=sq_send.at[slot], dst_ref=sq_recv.at[slot], send_sem=sqs.at[slot],
            recv_sem=sqr.at[slot], device_id={"head": other}, device_id_type=MESH,
        )

    def to_partner(turn, n):
        return pltpu.make_async_remote_copy(
            src_ref=send1.at[turn, n], dst_ref=recv1.at[turn, n], send_sem=s1.at[turn, n],
            recv_sem=r1.at[turn, n], device_id={"head": partner}, device_id_type=MESH,
        )

    def to_across(n):
        return pltpu.make_async_remote_copy(
            src_ref=send2.at[n], dst_ref=recv2.at[n], send_sem=s2.at[n],
            recv_sem=r2.at[n], device_id={"head": across}, device_id_type=MESH,
        )

    def block_of(slot):
        turn = slot // 2
        side = slot % 2
        row = (1 - turn) * (1 - half) + turn * half
        return row * 2 + (1 - side) * (1 - core) + side * core

    def rows_at(slot):
        return pl.ds(pl.multiple_of(block_of(slot) * SPAN, SPAN), SPAN)

    def columns_at(q):
        return pl.ds(pl.multiple_of(q * lanes, lanes), lanes)

    with jax.named_scope("A_local"):
        local_states()
    with jax.named_scope("B_barrier"):
        pl.semaphore_wait(barrier, 6)
    decay_copy().start()
    for q in range(pieces):
        final_copy(q).start()

    @pl.when(rank < 2)
    def _():
        came[...] = jnp.zeros_like(came)

    wide_skip = dot_nn(two_pieces(jnp.broadcast_to(skip_ref[...], (8, heads))), eye)[0:1]
    for q in range(pieces):
        part = slice(q * lanes, (q + 1) * lanes)
        eyes[q] = eye[:, part]
        skips[q] = wide_skip[:, part]
        gains[q] = gain_ref[:, part]
    squares[...] = jnp.zeros_like(squares)

    def tables(slot, _):
        rows = rows_at(slot)
        codes = code_ref[:, rows]
        parts = digits(codes, flag_ref[:, rows])
        upto = jnp.where(sj <= si, 1.0, 0.0).astype(BF16)
        sum_col, count_col = joined(dot_nt(upto, parts), heads, 1)
        sum_row, count_row = joined(dot_nt(parts, upto), heads, 0)
        cum_col = -rate_row * sum_col
        cum_row = -rate_col * sum_row
        for q in range(pieces):
            columns_of[slot, q] = cum_col[:, 2 * q : 2 * q + 2]
        for h in range(heads):
            rows_of[slot, h] = cum_row[h : h + 1, :]
        fall[slot] = two_pieces(jnp.where(count_col == 0.0, jnp.exp2(cum_col), 0.0))
        linked = (count_col[:, 0:1] == count_row[0:1, :]) & (sj <= si)
        cross[slot] = jnp.where(linked, dot_nt(c_ref[rows, :], b_ref[rows, :]), 0.0)
        wide = dot_nn(scales(codes).astype(BF16), eye[0:heads])
        scaled[rows, :] = (x_ref[rows, :].astype(F32) * wide).astype(BF16)
        return 0

    def intra(slot, q):
        both = scaled[rows_at(slot), columns_at(q)]
        lane = lax.broadcasted_iota(jnp.int32, (1, lanes), 1)
        left = jnp.where(lane < HEAD_DIM, 1.0, 0.0).astype(BF16)
        sides = (both * left, both * (1.0 - left))
        pair = columns_of[slot, q]
        upper, under = [], []
        for side in range(2):
            column = pair[:, side : side + 1]
            row = rows_of[slot, 2 * q + side]
            gap = jnp.minimum(column[0:lower] - row[:, 0:lower], 0.0)
            upper.append((jnp.exp2(gap) * cross[slot, 0:lower, 0:lower]).astype(BF16))
            gap = jnp.minimum(column[lower:] - row, 0.0)
            under.append((jnp.exp2(gap) * cross[slot, lower:, :]).astype(BF16))
        top = dot_nn(
            jnp.concatenate(upper, axis=1),
            jnp.concatenate([sides[0][0:lower], sides[1][0:lower]], axis=0),
        )
        bottom = dot_nn(jnp.concatenate(under, axis=1), jnp.concatenate(sides, axis=0))
        return jnp.concatenate([top, bottom], axis=0)

    def finish(slot, q, within):
        rows = rows_at(slot)
        part = columns_at(q)
        carried = dot_nn(c_ref[rows, :], starts[block_of(slot), q]) * dot_nn(fall[slot], eyes[q])
        gate = gate_ref[rows, part].astype(F32)
        total = within + carried + skips[q] * x_ref[rows, part].astype(F32)
        gated = total * (gate / (1.0 + jnp.exp(-gate)))
        mine[slot, :, part] = (gated * gains[q]).astype(BF16)
        squares[slot] = squares[slot] + gated * gated

    def send_squares(slot):
        value = squares[slot]
        high = value.astype(BF16)
        low = (value - high.astype(F32)).astype(BF16)
        ones = jnp.ones((8, lanes), BF16)
        sq_send[slot] = dot_nt(ones, high) + dot_nt(ones, low)

    def early(q, _):
        ssm[0, q] = intra(0, q)
        ssm[1, q] = intra(1, q)
        return 0

    with jax.named_scope("C_tables"):
        lax.fori_loop(0, 2, tables, 0)
    later_level = (level + shards) // (shards + 1)
    with jax.named_scope("D_early"):
        lax.fori_loop(0, EARLY + (pieces - EARLY) * later_level, early, 0)

    with jax.named_scope("E_decay"):
        decay_copy().wait_recv()
    for n in range(blocks):
        load_gate(n).wait()
    odd_f = odd.astype(F32)
    even_f = 1.0 - odd_f

    def chain(q, _):
        final_copy(q).wait_recv()

        @pl.when(rank >= 2)
        def _():
            chain_copy(q).wait_recv()

        ours = decay[q]
        theirs = other_decay[q]
        here = own[q]
        there = other_final[q].astype(F32)
        before = came[q].astype(F32)
        first = odd_f * there + even_f * here
        second = odd_f * here + even_f * there
        total = (odd_f * ours + even_f * theirs) * first + second
        passed[q] = (ours * theirs * before + total).astype(BF16)

        @pl.when(rank < shards - 2)
        def _():
            chain_copy(q).start()

        incoming = (odd_f * theirs + even_f) * before + odd_f * there
        for n in range(blocks):
            starts[n, q] = (local[n, q] + reach[n, q] * incoming).astype(BF16)

        @pl.when((level < 1) & (q < pieces - EARLY))
        def _():
            early(EARLY + q, 0)

        finish(0, q, ssm[0, q])
        finish(1, q, ssm[1, q])
        return 0

    with jax.named_scope("F_chain"):
        lax.fori_loop(0, pieces, chain, 0)
    with jax.named_scope("G_wload"):
        for n in range(CHUNKS):
            load(n).wait()

    def give(n):
        send1[0, n] = dot_nn(mine[0], w[n]).astype(BF16)
        to_partner(0, n).start()

    def cross_over(n):
        part = dot_nn(mine[1], w[n])
        with jax.named_scope("H_w"):
            to_partner(0, n).wait_recv()
        send2[n] = (part + recv1[0, n].astype(F32)).astype(BF16)
        to_across(n).start()

    def first(n, _):
        give(n)
        cross_over(n - 1)
        return 0

    with jax.named_scope("H_first"):
        give(0)
        lax.fori_loop(1, CHUNKS, first, 0)
        cross_over(CHUNKS - 1)
    send_squares(0)
    square_copy(0, diagonal).start()
    send_squares(1)
    square_copy(1, across).start()

    def rest(q, _):
        within = (intra(2, q), intra(3, q))
        finish(2, q, within[0])
        finish(3, q, within[1])
        return 0

    with jax.named_scope("I_rest"):
        lax.fori_loop(2, 4, tables, 0)
        lax.fori_loop(0, pieces, rest, 0)
    send_squares(2)
    square_copy(2, partner).start()
    send_squares(3)

    def third(n, _):
        send1[1, n] = dot_nn(mine[2], w[n]).astype(BF16)
        to_partner(1, n).start()
        return 0

    def fourth(n, _):
        part = dot_nn(mine[3], w[n])
        to_partner(1, n).wait_recv()
        kept[n] = part + recv1[1, n].astype(F32)
        return 0

    with jax.named_scope("J_third"):
        lax.fori_loop(0, CHUNKS, third, 0)
    with jax.named_scope("K_fourth"):
        lax.fori_loop(0, CHUNKS, fourth, 0)
    for slot, other in enumerate((diagonal, across, partner)):
        square_copy(slot, other).wait()
    total = (sq_send[3] + sq_recv[0] + sq_recv[1] + sq_recv[2])[0:1, :]
    norm = lax.rsqrt(total / (4 * inner) + 1e-05)
    column = jnp.sum(jnp.where(si == sj, norm, 0.0), axis=1, keepdims=True)
    for n in range(CHUNKS):
        with jax.named_scope("Q_across"):
            to_across(n).wait_recv()
        out_ref[:, n * width : (n + 1) * width] = (
            (kept[n] + recv2[n].astype(F32)) * column
        ).astype(BF16)
    for n in range(CHUNKS):
        to_partner(0, n).wait_send()
        to_partner(1, n).wait_send()
        to_across(n).wait_send()
    for q in range(pieces):
        final_copy(q).wait_send()
    decay_copy().wait_send()

    @pl.when(rank < shards - 2)
    def _():
        for q in range(pieces):
            chain_copy(q).wait_send()


def local(shards, xs, gate_branch, bmat, cmat, dt_code, resets, decay_rate, skip, norm_gain, out_weight):
    ticks, inner = xs.shape
    heads = dt_code.shape[0]
    size = bmat.shape[1]
    model = out_weight.shape[1]
    width = model // CHUNKS
    pieces = heads // 2
    blocks = ticks // SPAN
    lanes = 2 * HEAD_DIM
    vmem = pl.BlockSpec(memory_space=pltpu.VMEM)
    anywhere = pl.BlockSpec(memory_space=pl.ANY)
    dma = pltpu.SemaphoreType.DMA
    return pl.pallas_call(
        functools.partial(layer_kernel, shards),
        out_shape=pltpu.VMEM((SPAN, model), BF16),
        in_specs=[anywhere, anywhere] + [vmem] * 7 + [anywhere],
        out_specs=vmem,
        scratch_shapes=[
            pltpu.VMEM((ticks, inner), BF16),
            pltpu.VMEM((ticks, inner), BF16),
            pltpu.VMEM((CHUNKS, inner, width), BF16),
            pltpu.VMEM((ticks, inner), BF16),
            pltpu.VMEM((4, SPAN, SPAN), F32),
            pltpu.VMEM((4, pieces, SPAN, 2), F32),
            pltpu.VMEM((4, heads, 1, SPAN), F32),
            pltpu.VMEM((4, SPAN, 2 * heads), BF16),
            pltpu.VMEM((pieces, 2 * heads, lanes), BF16),
            pltpu.VMEM((pieces, 1, lanes), F32),
            pltpu.VMEM((pieces, 1, lanes), F32),
            pltpu.VMEM((blocks, pieces, 1, lanes), F32),
            pltpu.VMEM((blocks, pieces, size, lanes), F32),
            pltpu.VMEM((2, pieces, SPAN, lanes), F32),
            pltpu.VMEM((4, SPAN, inner), BF16),
            pltpu.VMEM((4, SPAN, lanes), F32),
            pltpu.VMEM((pieces, size, lanes), F32),
            pltpu.VMEM((pieces, size, lanes), BF16),
            pltpu.VMEM((pieces, size, lanes), BF16),
            pltpu.VMEM((pieces, 1, lanes), F32),
            pltpu.VMEM((pieces, 1, lanes), F32),
            pltpu.VMEM((pieces, size, lanes), BF16),
            pltpu.VMEM((pieces, size, lanes), BF16),
            pltpu.VMEM((blocks, pieces, size, lanes), BF16),
            pltpu.VMEM((CHUNKS, SPAN, width), F32),
            pltpu.VMEM((2, CHUNKS, SPAN, width), BF16),
            pltpu.VMEM((2, CHUNKS, SPAN, width), BF16),
            pltpu.VMEM((CHUNKS, SPAN, width), BF16),
            pltpu.VMEM((CHUNKS, SPAN, width), BF16),
            pltpu.VMEM((4, 8, SPAN), F32),
            pltpu.VMEM((3, 8, SPAN), F32),
            dma((blocks,)),
            dma((blocks,)),
            dma((CHUNKS,)),
            dma((pieces,)),
            dma((pieces,)),
            dma((1,)),
            dma((1,)),
            dma((pieces,)),
            dma((pieces,)),
            dma((2, CHUNKS)),
            dma((2, CHUNKS)),
            dma((CHUNKS,)),
            dma((CHUNKS,)),
            dma((3,)),
            dma((3,)),
        ],
        compiler_params=pltpu.CompilerParams(
            collective_id=0, has_side_effects=True, vmem_limit_bytes=VMEM_BYTES
        ),
        name="layer",
    )(
        xs, gate_branch, bmat, cmat, dt_code, resets[None, :], decay_rate[None, :], skip[None, :],
        norm_gain[None, :], out_weight,
    )


def solution(mesh):
    in_specs = (
        P("seq", "head"),
        P("seq", "head"),
        P("seq", None),
        P("seq", None),
        P("head", "seq"),
        P("seq"),
        P("head"),
        P("head"),
        P("head"),
        P("head", None),
    )
    out_specs = P(("seq", "head"), None)
    return jax.shard_map(
        functools.partial(local, mesh.shape["seq"]),
        mesh=mesh, in_specs=in_specs, out_specs=out_specs, check_vma=False,
    )
```
